256 devices in a mesh: row: 16 (over z, core), col: 16 (over y, x).
Axes of the slice: x: 4, y: 4, z: 8, core: 2. Of those that a mesh axis runs over, the one named last changes fastest.
Arguments:
- design: float32 [8192, 65536], P('row', 'col'), may hold values from -0.0625 to 0.0625
- targets: float32 [32, 8192], P(None, 'row'), may hold values from -6 to 6
- warm_solution: float32 [32, 65536], P(None, ('col', 'row')), may hold values from -2 to 2
- warm_sparse: float32 [32, 65536], P(None, ('col', 'row')), may hold values from -2 to 2
- warm_dual: float32 [32, 65536], P(None, ('col', 'row')), may hold values from -1.5 to 1.5
- sparsity: float32 [32], replicated, may hold values from 0.02 to 0.2
Outputs:
- solution: float32 [32, 65536], P(None, ('col', 'row'))
- sparse: float32 [32, 65536], P(None, ('col', 'row'))
- scaled_dual: float32 [32, 65536], P(None, ('col', 'row'))
The draws below stay inside these ranges and needn't reach their ends.
All inputs are finite; a program needn't handle non-finite values.
Results may differ from the reference program's by a relative error of at most 0.0003.
Values sent between devices are 32-bit elements; how exact they have to be, the bound alone decides.
No kernel may reach another device: no remote copies, remote signals or barrier semaphores. Data moves between devices by JAX's collectives and lax.ppermute only.
A program may use at most 64 MiB of HBM per device.

```python
import math
import jax
import jax.numpy as jnp
from jax import lax

N = 65536
K = 32
OUTER = 1
STEPS = 3
M = 8192


def strengthened(array, rng, source, target, shards_of, factor):
    owner, partner = [(jnp.arange(array.shape[position]) // (array.shape[position] // shards_of)).reshape([-1 if axis == position else 1 for axis in range(array.ndim)]) for position in (source, target)]
    chosen = jax.random.permutation(rng, shards_of)[partner]
    strong = (owner == chosen) | (owner == (partner + shards_of // 2) % shards_of)
    return jnp.where(strong, factor * array, array)


def block_scale(own_key, shape, pieces, least, top_value):
    def one(axis_at, shards_of):
        draws = jax.random.uniform(jax.random.fold_in(jax.random.fold_in(own_key, 6), axis_at), (shards_of,), jnp.float32, least / len(pieces), top_value / len(pieces))
        return jnp.repeat(jnp.exp(draws), shape[axis_at] // shards_of).reshape((-1,) + (1,) * (len(shape) - axis_at - 1))

    level = one(*pieces[0])
    for cut in pieces[1:]:
        level = level * one(*cut)
    return level


def bell_draw(stream_key, dims, deviation, limit, shards=(), dtype=jnp.bfloat16):
    array = jax.random.normal(stream_key, dims, jnp.float32) * deviation
    if len(shards) > 0:
        array = block_scale(stream_key, dims, shards, -0.22, 0.18) * array
    return jnp.clip(array, min=-limit, max=limit).astype(dtype)


def heavy_noise(stream_key, dims, spread, limit, split, heavy, dtype=jnp.bfloat16):
    values = spread * jax.random.normal(stream_key, dims, jnp.float32)
    if split:
        values = values * block_scale(stream_key, dims, split, -0.22, 0.18)
    return jnp.clip(strengthened(values, jax.random.fold_in(stream_key, 3), *heavy), -limit, limit).astype(dtype)


def setup_inputs(seed: int = 0) -> dict:
    key_list = jax.random.split(jax.random.key(seed), 7)
    design = heavy_noise(key_list[0], (M, N), (N // 4) ** -0.5, 0.0625, ((0, 16), (1, 16)), (0, 1, 16, 2.0), jnp.float32)
    targets = bell_draw(key_list[1], (K, M), 1.0, 6.0, ((1, 16),), jnp.float32)
    warm_solution = bell_draw(key_list[2], (K, N), 0.3, 2.0, ((1, 256),), jnp.float32)
    warm_sparse = bell_draw(key_list[3], (K, N), 0.3, 2.0, ((1, 256),), jnp.float32)
    warm_dual = bell_draw(key_list[4], (K, N), 0.2, 1.5, ((1, 256),), jnp.float32)
    sparsity = jnp.clip(jnp.exp(jax.random.uniform(key_list[5], (K,), jnp.float32, math.log(0.02), math.log(0.2))), 0.02, 0.2)
    return dict(design=design, targets=targets, warm_solution=warm_solution, warm_sparse=warm_sparse, warm_dual=warm_dual, sparsity=sparsity)


penalty = 0.5


def gram(design, vector):
    forward = lax.dot_general(vector, design, (((1,), (1,)), ((), ())), precision=lax.Precision.HIGHEST, preferred_element_type=jnp.float32)
    back = jnp.dot(forward, design, precision=lax.Precision.HIGHEST, preferred_element_type=jnp.float32)
    return back + penalty * vector


def reference(design, targets, warm_solution, warm_sparse, warm_dual, sparsity):
    fitted = jnp.dot(targets, design, precision=lax.Precision.HIGHEST, preferred_element_type=jnp.float32)
    thresh = (sparsity / penalty)[:, None]
    solution, sparse, scaled_dual = warm_solution, warm_sparse, warm_dual
    for outer in range(OUTER):
        rhs = fitted + penalty * (sparse - scaled_dual)
        residual = rhs - gram(design, solution)
        direction = residual
        norm_now = jnp.sum(residual * residual, axis=1, keepdims=True)
        for step in range(STEPS):
            image = gram(design, direction)
            alpha = norm_now / jnp.sum(direction * image, axis=1, keepdims=True)
            solution = solution + alpha * direction
            residual = residual - alpha * image
            norm_next = jnp.sum(residual * residual, axis=1, keepdims=True)
            direction = residual + (norm_next / norm_now) * direction
            norm_now = norm_next
        merged = solution + scaled_dual
        sparse = jnp.sign(merged) * jnp.maximum(jnp.abs(merged) - thresh, 0.0)
        scaled_dual = merged - sparse
    return solution, sparse, scaled_dual
```

```python
import jax
import jax.numpy as jnp
from jax import lax
from jax.sharding import Mesh
from jax.sharding import PartitionSpec as P

STEPS = 3
COL = ("col_0", "col_1")
ROW = ("row_0", "row_1")
COL_ROW = ("col_0", "col_1", "row_0", "row_1")

penalty = 0.5
Z = 8
K = 32
W = 512
H = 256


def pair(x):
    return lax.ppermute(x, "row_1", [(0, 1), (1, 0)])


def along_z(x, k):
    table = []
    for z in range(Z):
        table.append((2 * z, 2 * ((z + k) % Z)))
        table.append((2 * z + 1, 2 * ((z - k) % Z) + 1))
    return lax.ppermute(x, ROW, table)


def ring_sum(x, axis):
    n = 4
    far = lax.ppermute(x, axis, [(i, (i + 2) % n) for i in range(n)])
    up = lax.ppermute(x, axis, [(i, (i + 1) % n) for i in range(n)])
    down = lax.ppermute(x, axis, [(i, (i - 1) % n) for i in range(n)])
    return (x + up) + (down + far)


def plane_sum(x):
    return ring_sum(ring_sum(x, "col_1"), "col_0")


def dot_t(vector, block):
    return lax.dot_general(
        vector, block, (((1,), (1,)), ((), ())),
        precision=lax.Precision.HIGH, preferred_element_type=jnp.float32,
    )


def dot(values, block):
    return jnp.dot(values, block, precision=lax.Precision.HIGH, preferred_element_type=jnp.float32)


def row_sums(values):
    return jnp.sum(values, axis=1, keepdims=True)


def widened(*stats):
    lanes = lax.broadcasted_iota(jnp.int32, (K, 128), 1)
    out = jnp.zeros((K, 128), jnp.float32)
    for i, stat in enumerate(stats):
        out = jnp.where(lanes == i, stat, out)
    return out


def on_device(design, targets, warm_solution, warm_sparse, warm_dual, sparsity):
    z = lax.axis_index("row_0")
    core = lax.axis_index("row_1")
    sign = 1 - 2 * core

    def half(x, which):
        return lax.dynamic_slice_in_dim(x, which * H, H, 1)

    def joined(mine, other):
        return jnp.where(core == 0, jnp.concatenate([mine, other], 1), jnp.concatenate([other, mine], 1))

    def gathered(chip, extra):
        parts = {}
        small = half(chip, core)
        for k in (4, 3, 2, 1):
            body = small if k == 4 else chip
            parts[k] = along_z(body if extra is None else jnp.concatenate([body, extra], 1), k)
        mine = jnp.concatenate([parts[k] for k in (1, 2, 3, 4)], 1)
        theirs = pair(mine)
        step = W + (0 if extra is None else 128)
        a = [mine[:, i * step : i * step + W] for i in range(3)]
        q = [theirs[:, i * step : i * step + W] for i in range(3)]
        far = joined(mine[:, 3 * step : 3 * step + H], theirs[:, 3 * step : 3 * step + H])
        ordered = jnp.stack([chip, a[0], a[1], a[2], far, q[2], q[1], q[0]])
        whole = jnp.concatenate(
            [lax.dynamic_index_in_dim(ordered, (sign * (z - t)) % Z, 0, False) for t in range(Z)], 1
        )
        if extra is None:
            return whole, None
        total = extra + mine[:, 3 * step + H :]
        for i in range(3):
            total = total + (mine[:, i * step + W : (i + 1) * step] + theirs[:, i * step + W : (i + 1) * step])
        return whole, total

    def reduced(partial, extra):
        c = jnp.moveaxis(partial.reshape(K, Z, W), 1, 0)
        pick = lambda k: lax.dynamic_index_in_dim(c, (z + sign * k) % Z, 0, False)
        own, far = pick(0), pick(4)
        tail = [] if extra is None else [extra]
        keep = jnp.concatenate([pick(1), pick(2), pick(3), half(far, core), half(own, core)] + tail, 1)
        send = jnp.concatenate([pick(-1), pick(-2), pick(-3), half(far, 1 - core), half(own, 1 - core)] + tail, 1)
        both = keep + pair(send)
        got4 = along_z(both[:, 3 * W : 3 * W + H], 4)
        got3 = along_z(both[:, 2 * W : 3 * W], 3)
        got2 = along_z(both[:, W : 2 * W], 2)
        got1 = along_z(both[:, :W], 1)
        mine = got4 + both[:, 3 * W + H : 4 * W]
        side = (got1 + got2 + got3) + joined(mine, jnp.zeros_like(mine))
        chip = side + pair(side)
        return chip, (None if extra is None else both[:, 4 * W :])

    shift = warm_sparse - warm_dual - warm_solution
    mine = jnp.concatenate([warm_solution, shift], 0)
    both = joined(mine, pair(mine))
    whole, _ = gathered(both[:K], None)
    values = targets - plane_sum(dot_t(whole, design))
    chip, _ = reduced(dot(values, design), None)
    chip = chip + penalty * both[K:]
    residual, _ = gathered(chip, None)
    own_residual = half(chip, core)

    solution = warm_solution
    direction = image = None
    for step in range(STEPS):
        stats = [row_sums(residual * residual)]
        if step:
            stats.append(row_sums(residual * direction))
        payload = jnp.concatenate([dot_t(residual, design), widened(*stats)], 1)
        payload = plane_sum(payload)
        values, norm = payload[:, :W], payload[:, W : W + 1]
        if step == 0:
            direction, own_direction, image, square = residual, own_residual, values, norm
        else:
            ratio = norm / norm_before
            square = norm + ratio * (2.0 * payload[:, W + 1 : W + 2] + ratio * square)
            image = values + ratio * image
            direction = residual + ratio * direction
            own_direction = own_residual + ratio * own_direction
        norm_before = norm
        part = widened(row_sums(image * image))
        if step + 1 < STEPS:
            chip, part = reduced(dot(image, design), part)
            back, part = gathered(chip, part)
        else:
            part = part + pair(part)
            sent = {k: along_z(part, k) for k in (4, 3, 2, 1)}
            side = (sent[1] + sent[2]) + (sent[3] + 0.5 * sent[4])
            part = part + (side + pair(side))
        alpha = norm / (part[:, :1] + penalty * square)
        solution = solution + alpha * own_direction
        if step + 1 < STEPS:
            residual = residual - alpha * (back + penalty * direction)
            own_residual = own_residual - alpha * (half(chip, core) + penalty * own_direction)

    thresh = (sparsity / penalty)[:, None]
    merged = solution + warm_dual
    sparse = jnp.sign(merged) * jnp.maximum(jnp.abs(merged) - thresh, 0.0)
    return solution, sparse, merged - sparse


def solution(mesh):
    finer = Mesh(mesh.devices.reshape(8, 2, 4, 4), ("row_0", "row_1", "col_0", "col_1"))
    return jax.shard_map(
        on_device,
        mesh=finer,
        in_specs=(
            P(ROW, COL),
            P(None, ROW),
            P(None, COL_ROW),
            P(None, COL_ROW),
            P(None, COL_ROW),
            P(),
        ),
        out_specs=(P(None, COL_ROW), P(None, COL_ROW), P(None, COL_ROW)),
        check_vma=False,
    )
```

```python
import functools

import jax
import jax.numpy as jnp
from jax import lax
from jax.experimental import pallas as pl
from jax.experimental.pallas import tpu as pltpu
from jax.sharding import Mesh
from jax.sharding import PartitionSpec as P

STEPS = 3
COL = ("col_0", "col_1")
ROW = ("row_0", "row_1")
COL_ROW = ("col_0", "col_1", "row_0", "row_1")

penalty = 0.5
Z = 8
K = 32
W = 512
H = 256
S = 128
UNROLL = 1


def pair(x):
    return lax.ppermute(x, "row_1", [(0, 1), (1, 0)])


def along_z(x, k):
    table = []
    for z in range(Z):
        table.append((2 * z, 2 * ((z + k) % Z)))
        table.append((2 * z + 1, 2 * ((z - k) % Z) + 1))
    return lax.ppermute(x, ROW, table)


def across(x, turn, k):
    table = []
    for core in range(2):
        for a in range(4):
            for b in range(4):
                if core == turn:
                    to = (a, (b + k) % 4)
                else:
                    to = ((a + k) % 4, b)
                table.append((core * 16 + a * 4 + b, core * 16 + to[0] * 4 + to[1]))
    return lax.ppermute(x, ("row_1",) + COL, table)


def ring_parts(x, turn):
    far = across(x, turn, 2)
    return x, across(x, turn, 1), across(x, turn, 3), far


def split(x):
    hi = x.astype(jnp.bfloat16)
    return hi, (x - hi.astype(jnp.float32)).astype(jnp.bfloat16)


def dot(a, b, transposed):
    dims = (((1,), (1 if transposed else 0,)), ((), ()))
    return lax.dot_general(a, b, dims, preferred_element_type=jnp.float32)


def product(both, block, transposed):
    hi, lo = split(block)
    wide = dot(both, hi, transposed)
    return (wide[:K] + wide[K:]) + dot(both[:K], lo, transposed)


def fetches(place, design, blocks, sems, offsets):
    z, sign = place[0], place[1]
    copies = []
    for j, offset in enumerate(offsets):
        at = pl.multiple_of(lax.rem(z + sign * offset + 2 * Z, Z) * W, W)
        copies.append(pltpu.make_async_copy(design.at[:, pl.ds(at, W)], blocks.at[j], sems.at[j]))
    return copies


def lanes(*stats):
    lane = lax.broadcasted_iota(jnp.int32, (K, S), 1)
    out = jnp.zeros((K, S), jnp.float32)
    for i, stat in enumerate(stats):
        out = jnp.where(lane == i, stat, out)
    return out


def row_sums(values):
    return jnp.sum(values, axis=1, keepdims=True)


F_OFFSETS = (0, -1, -2, -3, 4, 3, 2, 1)
B_OFFSETS = (-1, -2, -3, 4, 0, 1, 2, 3)


def forward_kernel(mode, *refs):
    refs = list(refs)
    take = lambda n: [refs.pop(0) for _ in range(n)]
    place, design, chip, mine, theirs = take(5)
    if mode == 2:
        state, part, before, direction, found = take(5)
    (out,) = take(1)
    if mode:
        (after,) = take(1)
    if mode == 2:
        (found_out,) = take(1)
    blocks, both, acc, sems = take(4)
    copies = fetches(place, design, blocks, sems, F_OFFSETS)
    for copy in copies:
        copy.start()
    step = W + (S if mode == 2 else 0)
    if mode == 2:
        total = part[...] + mine[:, 3 * step + H :]
        for i in range(3):
            total = total + (mine[:, i * step + W : (i + 1) * step] + theirs[:, i * step + W : (i + 1) * step])
        alpha = state[:, 0:1] / (total[:, 0:1] + penalty * state[:, 1:2])
        found_out[...] = found[...] + alpha * direction[0]
    squares = crossed = None
    for j in range(Z):
        if j == 0:
            value = chip[...]
        elif j < 4:
            value = mine[:, (j - 1) * step : (j - 1) * step + W]
        elif j > 4:
            value = theirs[:, (7 - j) * step : (7 - j) * step + W]
        else:
            a, b = mine[:, 3 * step : 3 * step + H], theirs[:, 3 * step : 3 * step + H]
            first = place[2] == 0
            value = jnp.concatenate([jnp.where(first, a, b), jnp.where(first, b, a)], 1)
        if mode == 2:
            old = direction[j]
            value = before[j] - alpha * (value + penalty * old)
            crossed = value * old if crossed is None else crossed + value * old
        if mode:
            after[j] = value
            squares = value * value if squares is None else squares + value * value
        hi, lo = split(value)
        both[j, :K] = hi
        both[j, K:] = lo
    acc[...] = jnp.zeros_like(acc)

    def body(j, carry):
        pltpu.make_async_copy(design.at[:, pl.ds(0, W)], blocks.at[j], sems.at[j]).wait()
        acc[...] += product(both[j], blocks[j], True)
        return carry

    lax.fori_loop(0, Z, body, 0, unroll=UNROLL)
    if mode:
        out[:, :W] = acc[...]
        stats = [row_sums(squares)] + ([row_sums(crossed)] if mode == 2 else [])
        out[:, W:] = lanes(*stats)
    else:
        out[...] = acc[...]


def backward_kernel(mode, *refs):
    refs = list(refs)
    take = lambda n: [refs.pop(0) for _ in range(n)]
    place, design, a, b, c, d = take(6)
    if mode == 0:
        (targets,) = take(1)
    if mode == 2:
        state, image, after, direction = take(4)
    keep, send = take(2)
    if mode:
        image_out, state_out = take(2)
    if mode == 2:
        (direction_out,) = take(1)
    blocks, outs, sems = take(3)
    copies = fetches(place, design, blocks, sems, B_OFFSETS)
    for copy in copies:
        copy.start()
    payload = (a[...] + b[...]) + (c[...] + d[...])
    if mode == 0:
        values = targets[...] - payload
    else:
        values = payload[:, :W]
        norm = payload[:, W : W + 1]
        square = norm
        if mode == 2:
            ratio = norm / state[:, 0:1]
            square = norm + ratio * (2.0 * payload[:, W + 1 : W + 2] + ratio * state[:, 1:2])
            values = values + ratio * image[...]
            for j in range(Z):
                direction_out[j] = after[j] + ratio * direction[j]
        image_out[...] = values
        state_out[...] = lanes(norm, square)
        part = lanes(row_sums(values * values))
        keep[:, 4 * W :] = part
        send[:, 4 * W :] = part
    hi, lo = split(values)
    both = jnp.concatenate([hi, lo], 0)

    def body(j, carry):
        pltpu.make_async_copy(design.at[:, pl.ds(0, W)], blocks.at[j], sems.at[j]).wait()
        outs[j] = product(both, blocks[j], False)
        return carry

    lax.fori_loop(0, Z, body, 0, unroll=UNROLL)
    first = place[2] == 0
    for i in range(3):
        send[:, i * W : (i + 1) * W] = outs[i]
        keep[:, i * W : (i + 1) * W] = outs[5 + i]
    for i in range(2):
        one, two = outs[3 + i, :, :H], outs[3 + i, :, H:]
        at = 3 * W + i * H
        keep[:, at : at + H] = jnp.where(first, one, two)
        send[:, at : at + H] = jnp.where(first, two, one)


VMEM = pl.BlockSpec(memory_space=pltpu.VMEM)
SMEM = pl.BlockSpec(memory_space=pltpu.SMEM)
ANY = pl.BlockSpec(memory_space=pl.ANY)


def array(*shape):
    return jax.ShapeDtypeStruct(shape, jnp.float32)


def call(kernel, mode, place, design, args, outs, scratch):
    return pl.pallas_call(
        functools.partial(kernel, mode),
        in_specs=[SMEM, ANY] + [VMEM] * len(args),
        out_specs=[VMEM] * len(outs),
        out_shape=outs,
        scratch_shapes=scratch,
        compiler_params=pltpu.CompilerParams(vmem_limit_bytes=24 * 1024 * 1024),
    )(place, design, *args)


BLOCKS = pltpu.VMEM((Z, W, W), jnp.float32)
SEMS = pltpu.SemaphoreType.DMA((Z,))


def forward(mode, place, design, *args):
    outs = [array(K, W + (S if mode else 0))]
    if mode:
        outs.append(array(Z, K, W))
    if mode == 2:
        outs.append(array(K, W))
    scratch = [BLOCKS, pltpu.VMEM((Z, 2 * K, W), jnp.bfloat16), pltpu.VMEM((K, W), jnp.float32), SEMS]
    return call(forward_kernel, mode, place, design, args, outs, scratch)


def backward(mode, place, design, *args):
    wide = 4 * W + (S if mode else 0)
    outs = [array(K, wide), array(K, wide)]
    if mode:
        outs += [array(K, W), array(K, S)]
    if mode == 2:
        outs.append(array(Z, K, W))
    scratch = [BLOCKS, pltpu.VMEM((Z, K, W), jnp.float32), SEMS]
    return call(backward_kernel, mode, place, design, args, outs, scratch)


def on_device(design, targets, warm_solution, warm_sparse, warm_dual, sparsity):
    z = lax.axis_index("row_0")
    core = lax.axis_index("row_1")
    place = jnp.stack([z, 1 - 2 * core, core]).astype(jnp.int32)

    def half(x):
        return jnp.where(core == 0, x[:, :H], x[:, H : 2 * H])

    def joined(mine, other):
        return jnp.where(core == 0, jnp.concatenate([mine, other], 1), jnp.concatenate([other, mine], 1))

    def gathered(chip, extra):
        tail = [] if extra is None else [extra]
        whole = jnp.concatenate([chip] + tail, 1)
        small = jnp.concatenate([half(chip)] + tail, 1)
        parts = {k: along_z(small if k == 4 else whole, k) for k in (4, 3, 2, 1)}
        mine = jnp.concatenate([parts[k] for k in (1, 2, 3, 4)], 1)
        return mine, pair(mine)

    def reduced(keep, send):
        both = keep + pair(send)
        got4 = along_z(both[:, 3 * W : 3 * W + H], 4)
        got3 = along_z(both[:, 2 * W : 3 * W], 3)
        got2 = along_z(both[:, W : 2 * W], 2)
        got1 = along_z(both[:, :W], 1)
        mine = got4 + both[:, 3 * W + H : 4 * W]
        side = (got1 + got2 + got3) + joined(mine, jnp.zeros_like(mine))
        return side + pair(side), both[:, 4 * W :]

    def plane(x):
        a, b, c, d = ring_parts(x, 0)
        return ring_parts((a + b) + (c + d), 1)

    start = jnp.concatenate([warm_solution, warm_sparse - warm_dual - warm_solution], 0)
    start = joined(start, pair(start))
    found = start[:K]
    (value,) = forward(0, place, design, found, *gathered(found, None))
    keep, send = backward(0, place, design, *plane(value), targets)
    chip, _ = reduced(keep, send)
    chip = chip + penalty * start[K:]
    value, residual = forward(1, place, design, chip, *gathered(chip, None))
    keep, send, image, state = backward(1, place, design, *plane(value))
    direction = residual
    for step in range(1, STEPS):
        chip, part = reduced(keep, send)
        mine, theirs = gathered(chip, part)
        value, residual, found = forward(
            2, place, design, chip, mine, theirs, state, part, residual, direction, found
        )
        parts = plane(value)
        if step + 1 < STEPS:
            keep, send, image, state, direction = backward(
                2, place, design, *parts, state, image, residual, direction
            )
    payload = (parts[0] + parts[1]) + (parts[2] + parts[3])
    norm = payload[:, W : W + 1]
    ratio = norm / state[:, 0:1]
    square = norm + ratio * (2.0 * payload[:, W + 1 : W + 2] + ratio * state[:, 1:2])
    image = payload[:, :W] + ratio * image
    direction = half(residual[0]) + ratio * half(direction[0])
    part = jnp.broadcast_to(row_sums(image * image), (K, S))
    part = part + pair(part)
    sent = {k: along_z(part, k) for k in (4, 3, 2, 1)}
    side = (sent[1] + sent[2]) + (sent[3] + 0.5 * sent[4])
    part = part + (side + pair(side))
    solution = half(found) + norm / (part[:, :1] + penalty * square) * direction

    thresh = (sparsity / penalty)[:, None]
    merged = solution + warm_dual
    sparse = jnp.sign(merged) * jnp.maximum(jnp.abs(merged) - thresh, 0.0)
    return solution, sparse, merged - sparse


def solution(mesh):
    finer = Mesh(mesh.devices.reshape(8, 2, 4, 4), ("row_0", "row_1", "col_0", "col_1"))
    return jax.shard_map(
        on_device,
        mesh=finer,
        in_specs=(
            P(ROW, COL),
            P(None, ROW),
            P(None, COL_ROW),
            P(None, COL_ROW),
            P(None, COL_ROW),
            P(),
        ),
        out_specs=(P(None, COL_ROW), P(None, COL_ROW), P(None, COL_ROW)),
        check_vma=False,
    )
```

```python
import functools

import jax
import jax.numpy as jnp
from jax import lax
from jax.experimental import pallas as pl
from jax.experimental.pallas import tpu as pltpu
from jax.sharding import Mesh
from jax.sharding import PartitionSpec as P

STEPS = 3
COL = ("col_0", "col_1")
ROW = ("row_0", "row_1")
COL_ROW = ("col_0", "col_1", "row_0", "row_1")

penalty = 0.5
Z = 8
K = 32
W = 512
H = 256
S = 128


def pair(x):
    return lax.ppermute(x, "row_1", [(0, 1), (1, 0)])


def along_z(x, k):
    table = []
    for z in range(Z):
        table.append((2 * z, 2 * ((z + k) % Z)))
        table.append((2 * z + 1, 2 * ((z - k) % Z) + 1))
    return lax.ppermute(x, ROW, table)


def ring_parts(x, axis):
    n = 4
    far = lax.ppermute(x, axis, [(i, (i + 2) % n) for i in range(n)])
    up = lax.ppermute(x, axis, [(i, (i + 1) % n) for i in range(n)])
    down = lax.ppermute(x, axis, [(i, (i - 1) % n) for i in range(n)])
    return x, up, down, far


def split(x):
    hi = x.astype(jnp.bfloat16)
    return hi, (x - hi.astype(jnp.float32)).astype(jnp.bfloat16)


def dot(a, b, transposed):
    dims = (((1,), (1 if transposed else 0,)), ((), ()))
    return lax.dot_general(a, b, dims, preferred_element_type=jnp.float32)


def product(both, hi, lo, transposed):
    wide = dot(both, hi, transposed)
    return (wide[:K] + wide[K:]) + dot(both[:K], lo, transposed)


def columns(place, offset):
    at = lax.rem(place[0] + place[1] * offset + 2 * Z, Z)
    return pl.ds(pl.multiple_of(at * W, W), W)


def lanes(*stats):
    lane = lax.broadcasted_iota(jnp.int32, (K, S), 1)
    out = jnp.zeros((K, S), jnp.float32)
    for i, stat in enumerate(stats):
        out = jnp.where(lane == i, stat, out)
    return out


def row_sums(values):
    return jnp.sum(values, axis=1, keepdims=True)


def forward_offset(j):
    return Z - j


def forward_kernel(
    place, hi, lo, chip, mine, theirs, state, part, before, direction, found,
    out, after, found_out, both, acc, top,
):
    step = W + S
    early = place[3] < 2
    total = part[...] + mine[:, 3 * step + H :]
    for i in range(3):
        total = total + (mine[:, i * step + W : (i + 1) * step] + theirs[:, i * step + W : (i + 1) * step])
    alpha = state[:, 0:1] / (total[:, 0:1] + penalty * state[:, 1:2])
    alpha = jnp.where(early, -1.0, alpha)
    kept = jnp.where(early, 0.0, 1.0)
    found_out[...] = found[...] + alpha * direction[0]
    first = place[2] == 0
    R = 16
    tops = []
    for i in range(K // R):
        rows = pl.ds(i * R, R)
        squares = crossed = None
        for j in range(Z):
            if j == 0:
                value = chip[rows, :]
            elif j < 4:
                value = mine[rows, (j - 1) * step : (j - 1) * step + W]
            elif j > 4:
                value = theirs[rows, (7 - j) * step : (7 - j) * step + W]
            else:
                a, b = mine[rows, 3 * step : 3 * step + H], theirs[rows, 3 * step : 3 * step + H]
                value = jnp.concatenate([jnp.where(first, a, b), jnp.where(first, b, a)], 1)
            old = direction[j, rows, :]
            value = kept * before[j, rows, :] - alpha[i * R : i * R + R] * (value + penalty * old)
            after[j, rows, :] = value
            squares = value * value if squares is None else squares + value * value
            crossed = value * old if crossed is None else crossed + value * old
            big, small = split(value)
            at = columns(place, forward_offset(j))
            both[rows, at] = big
            both[pl.ds(K + i * R, R), at] = small
        tops.append([row_sums(squares), row_sums(crossed)])
    acc[:, : 2 * K] = dot(hi[...], both[...], True)
    acc[:, 2 * K : 3 * K] = dot(lo[...], both[:K], True)
    top[...] = jnp.transpose(acc[...])
    out[:, :W] = (top[:K] + top[K : 2 * K]) + top[2 * K : 3 * K]
    out[:, W:] = lanes(*[jnp.concatenate(list(pieces), 0) for pieces in zip(*tops)])


def chunks(place, hi, lo, values, side, which, out):
    both = jnp.concatenate(split(values), 0)
    for i in range(3):
        at = columns(place, side * (i + 1))
        out[:, i * W : (i + 1) * W] = product(both, hi[:, at], lo[:, at], False)
    for i in range(2):
        start = lax.rem(place[0] + Z // 2 * (1 - i), Z) * W + which * H
        at = pl.ds(pl.multiple_of(start, H), H)
        spot = 3 * W + i * H
        out[:, spot : spot + H] = product(both, hi[:, at], lo[:, at], False)
    out[:, 4 * W :] = lanes(row_sums(values * values))


def send_kernel(place, hi, lo, a, b, c, d, state, image, send, image_out, state_out):
    turn = place[3]
    payload = (a[...] + b[...]) + (c[...] + d[...])
    norm = payload[:, W : W + 1]
    ratio = norm / state[:, 0:1]
    ratio = jnp.where(turn == 0, 1.0, jnp.where(turn == 1, 0.0, ratio))
    square = norm + ratio * (2.0 * payload[:, W + 1 : W + 2] + ratio * state[:, 1:2])
    values = jnp.where(turn == 0, -1.0, 1.0) * payload[:, :W] + ratio * image[...]
    image_out[...] = values
    state_out[...] = lanes(norm, square, ratio)
    chunks(place, hi, lo, values, -1, 1 - place[2], send)


def keep_kernel(place, hi, lo, state, image, after, direction, keep, direction_out):
    fresh = jnp.where(place[3] == 0, 0.0, 1.0)
    ratio = state[:, 2:3]
    for j in range(Z):
        direction_out[j] = fresh * after[j] + ratio * direction[j]
    chunks(place, hi, lo, image[...], 1, place[2], keep)


VMEM = pl.BlockSpec(memory_space=pltpu.VMEM)
SMEM = pl.BlockSpec(memory_space=pltpu.SMEM)
ANY = pl.BlockSpec(memory_space=pl.ANY)


def array(*shape):
    return jax.ShapeDtypeStruct(shape, jnp.float32)


def call(kernel, kinds, outs, scratch, limit, *args, flops=10**9):
    return pl.pallas_call(
        kernel,
        in_specs=kinds + [VMEM] * (len(args) - len(kinds)),
        out_specs=[VMEM] * len(outs),
        out_shape=outs,
        scratch_shapes=scratch,
        cost_estimate=pl.CostEstimate(flops=flops, transcendentals=0, bytes_accessed=2**23),
        compiler_params=pltpu.CompilerParams(vmem_limit_bytes=limit * 2**20),
    )(*args)


STACK = array(Z, K, W)
TERM = jax.ShapeDtypeStruct((W, Z * W), jnp.bfloat16)
WIDE = array(K, 4 * W + S)


def prepare_kernel(design, hi, lo):
    for i in range(0, W, 64):
        hi[i : i + 64], lo[i : i + 64] = split(design[i : i + 64])


def prepare(design):
    block = pl.BlockSpec((W, 2 * W), lambda j: (0, j))
    return pl.pallas_call(
        prepare_kernel,
        grid=(Z // 2,),
        in_specs=[block],
        out_specs=[block, block],
        out_shape=[TERM, TERM],
        cost_estimate=pl.CostEstimate(flops=10**10, transcendentals=0, bytes_accessed=2**24),
        compiler_params=pltpu.CompilerParams(vmem_limit_bytes=58 * 2**20),
    )(design)


def pack_kernel(place, chip, extra, whole, small):
    whole[:, :W] = chip[...]
    whole[:, W:] = extra[...]
    small[:, :H] = jnp.where(place[2] == 0, chip[:, :H], chip[:, H:])
    small[:, H:] = extra[...]


def forward(*args):
    scratch = [
        pltpu.VMEM((2 * K, Z * W), jnp.bfloat16),
        pltpu.VMEM((W, 4 * K), jnp.float32),
        pltpu.VMEM((4 * K, W), jnp.float32),
    ]
    return call(forward_kernel, [SMEM], [array(K, W + S), STACK, array(K, W)], scratch, 24, *args)


def on_device(design, targets, warm_solution, warm_sparse, warm_dual, sparsity):
    z = lax.axis_index("row_0")
    core = lax.axis_index("row_1")

    def place(turn):
        return jnp.stack([z, 1 - 2 * core, core, turn]).astype(jnp.int32)

    def half(x):
        return jnp.where(core == 0, x[:, :H], x[:, H : 2 * H])

    def joined(mine, other):
        return jnp.where(core == 0, jnp.concatenate([mine, other], 1), jnp.concatenate([other, mine], 1))

    def gathered(at, chip, extra):
        outs = [array(K, W + S), array(K, H + S)]
        whole, small = call(pack_kernel, [SMEM], outs, [], 24, at, chip, extra, flops=10**11)
        parts = {k: along_z(small if k == 4 else whole, k) for k in (4, 3, 2, 1)}
        mine = jnp.concatenate([parts[k] for k in (1, 2, 3, 4)], 1)
        return mine, pair(mine)

    def reduced(both):
        got4 = along_z(both[:, 3 * W : 3 * W + H], 4)
        got3 = along_z(both[:, 2 * W : 3 * W], 3)
        got2 = along_z(both[:, W : 2 * W], 2)
        got1 = along_z(both[:, :W], 1)
        mine = got4 + both[:, 3 * W + H : 4 * W]
        side = (got1 + got2 + got3) + joined(mine, jnp.zeros_like(mine))
        return side + pair(side), both[:, 4 * W :]

    def plane(x):
        a, b, c, d = ring_parts(x, "col_1")
        return ring_parts((a + b) + (c + d), "col_0")

    found = joined(warm_solution, pair(warm_solution))
    shift = penalty * (warm_sparse - warm_dual - warm_solution)
    shift = joined(shift, pair(shift))
    none = jnp.zeros((K, S), jnp.float32)
    stack = jnp.zeros((Z, K, W), jnp.float32)

    hi, lo = prepare(design)

    def ahead(turn, carry):
        chip, part, state, residual, direction, found, _ = carry
        at = place(turn)
        mine, theirs = gathered(at, chip, part)
        value, residual, found = forward(
            at, hi, lo, chip, mine, theirs, state, part, residual, direction, found
        )
        return at, plane(value), residual, found

    def advance(turn, carry):
        at, parts, residual, found = ahead(turn, carry)
        state, direction, image = carry[2], carry[4], carry[6]
        outs = [WIDE, array(K, W), array(K, S)]
        send, image, state = call(send_kernel, [SMEM], outs, [], 24, at, hi, lo, *parts, state, image)
        theirs = pair(send)
        keep, direction = call(
            keep_kernel, [SMEM], [WIDE, STACK], [], 24, at, hi, lo, state, image, residual, direction
        )
        chip, part = reduced(keep + theirs)
        chip = chip + jnp.where(turn == 0, shift, 0.0)
        return chip, part, state, residual, direction, found, image

    carry = lax.fori_loop(0, STEPS, advance, (found, none, none, stack, stack, found, targets))
    state, direction, image = carry[2], carry[4], carry[6]
    at, parts, residual, found = ahead(STEPS, carry)
    payload = (parts[0] + parts[1]) + (parts[2] + parts[3])
    norm = payload[:, W : W + 1]
    ratio = norm / state[:, 0:1]
    square = norm + ratio * (2.0 * payload[:, W + 1 : W + 2] + ratio * state[:, 1:2])
    image = payload[:, :W] + ratio * image
    direction = half(residual[0]) + ratio * half(direction[0])
    part = jnp.pad(row_sums(image * image)[:, 0], (0, S - K))
    sent = lax.all_to_all(jnp.broadcast_to(part, (16, 8, S)), ROW, 0, 0, tiled=True)
    part = jnp.sum(sent, axis=0)[0, :K, None]
    solution = half(found) + norm / (part + penalty * square) * direction

    thresh = (sparsity / penalty)[:, None]
    merged = solution + warm_dual
    sparse = jnp.sign(merged) * jnp.maximum(jnp.abs(merged) - thresh, 0.0)
    return solution, sparse, merged - sparse


def solution(mesh):
    finer = Mesh(mesh.devices.reshape(8, 2, 4, 4), ("row_0", "row_1", "col_0", "col_1"))
    return jax.shard_map(
        on_device,
        mesh=finer,
        in_specs=(
            P(ROW, COL),
            P(None, ROW),
            P(None, COL_ROW),
            P(None, COL_ROW),
            P(None, COL_ROW),
            P(),
        ),
        out_specs=(P(None, COL_ROW), P(None, COL_ROW), P(None, COL_ROW)),
        check_vma=False,
    )
```

```python
import jax
import jax.numpy as jnp
from jax import lax
from jax.experimental import pallas as pl
from jax.experimental.pallas import tpu as pltpu
from jax.sharding import Mesh
from jax.sharding import PartitionSpec as P


STEPS = 3
COL = ("col_0", "col_1")
ROW = ("row_0", "row_1")
COL_ROW = ("col_0", "col_1", "row_0", "row_1")

penalty = 0.5
Z = 8
K = 32
W = 512
H = 256
S = 128
T = 4 * K + 8


def pair(x):
    return lax.ppermute(x, "row_1", [(0, 1), (1, 0)])


def along_z(x, k):
    table = []
    for z in range(Z):
        table.append((2 * z, 2 * ((z + k) % Z)))
        table.append((2 * z + 1, 2 * ((z - k) % Z) + 1))
    return lax.ppermute(x, ROW, table)


def ring_parts(x, axis):
    n = 4
    parts = [x]
    for k in (2, 1, 3):
        parts.append(lax.ppermute(x, axis, [(i, (i + k) % n) for i in range(n)]))
    return parts


def split(x):
    hi = x.astype(jnp.bfloat16)
    return hi, (x - hi.astype(jnp.float32)).astype(jnp.bfloat16)


def dot(a, b, transposed):
    dims = (((1,), (1 if transposed else 0,)), ((), ()))
    return lax.dot_general(a, b, dims, preferred_element_type=jnp.float32)


def product(both, hi, lo, transposed):
    wide = dot(both, hi, transposed)
    return (wide[:K] + wide[K:]) + dot(both[:K], lo, transposed)


def columns(place, offset):
    at = lax.rem(place[0] + place[1] * offset + 2 * Z, Z)
    return pl.ds(pl.multiple_of(at * W, W), W)


def lanes(*stats):
    lane = lax.broadcasted_iota(jnp.int32, (K, S), 1)
    out = jnp.zeros((K, S), jnp.float32)
    for i, stat in enumerate(stats):
        out = jnp.where(lane == i, stat, out)
    return out


def flipped(stats):
    return jnp.transpose(jnp.concatenate([stats, jnp.zeros((S - K, S), jnp.float32)], 0))[:8]


def restored(tile):
    return jnp.transpose(jnp.concatenate([tile, jnp.zeros((S - 8, S), jnp.float32)], 0))[:K]


def row_sums(values):
    return jnp.sum(values, axis=1, keepdims=True)


def forward_offset(j):
    return Z - j


def forward_kernel(
    place, hi, lo, chip, mine, theirs, state, part, before, direction, found,
    out, after, found_out, both, acc, top,
):
    early = place[3] < 2
    total = mine[3 * T + 2 * K :]
    for i in range(3):
        at = slice(i * T + 4 * K, (i + 1) * T)
        total = total + (mine[at] + theirs[at])
    total = part[...] + restored(total)
    alpha = state[:, 0:1] / (total[:, 0:1] + penalty * state[:, 1:2])
    alpha = jnp.where(early, -1.0, alpha)
    kept = jnp.where(early, 0.0, 1.0)
    found_out[...] = found[...] + alpha * direction[0]
    first = place[2] == 0
    R = 16
    tops = []

    def piece(ref, index, count, i):
        starts = [index * T + c * K + i * R for c in range(count)]
        return jnp.concatenate([ref[at : at + R] for at in starts], 1)

    for i in range(K // R):
        rows = pl.ds(i * R, R)
        squares = crossed = None
        for j in range(Z):
            if j == 0:
                value = chip[rows, :]
            elif j < 4:
                value = piece(mine, j - 1, 4, i)
            elif j > 4:
                value = piece(theirs, 7 - j, 4, i)
            else:
                a, b = piece(mine, 3, 2, i), piece(theirs, 3, 2, i)
                value = jnp.concatenate([jnp.where(first, a, b), jnp.where(first, b, a)], 1)
            old = direction[j, rows, :]
            value = kept * before[j, rows, :] - alpha[i * R : i * R + R] * (value + penalty * old)
            after[j, rows, :] = value
            squares = value * value if squares is None else squares + value * value
            crossed = value * old if crossed is None else crossed + value * old
            big, small = split(value)
            at = columns(place, forward_offset(j))
            both[rows, at] = big
            both[pl.ds(K + i * R, R), at] = small
        tops.append([row_sums(squares), row_sums(crossed)])
    acc[:, : 2 * K] = dot(hi[...], both[...], True)
    acc[:, 2 * K : 3 * K] = dot(lo[...], both[:K], True)
    top[...] = jnp.transpose(acc[...])
    value = (top[:K] + top[K : 2 * K]) + top[2 * K : 3 * K]
    for c in range(4):
        out[c * K : (c + 1) * K] = value[:, c * S : (c + 1) * S]
    out[4 * K :] = flipped(lanes(*[jnp.concatenate(list(pieces), 0) for pieces in zip(*tops)]))


def chunks(place, hi, lo, values, side, which, out):
    both = jnp.concatenate(split(values), 0)
    for i in range(3):
        at = columns(place, side * (i + 1))
        out[:, i * W : (i + 1) * W] = product(both, hi[:, at], lo[:, at], False)
    for i in range(2):
        start = lax.rem(place[0] + Z // 2 * (1 - i), Z) * W + which * H
        at = pl.ds(pl.multiple_of(start, H), H)
        spot = 3 * W + i * H
        out[:, spot : spot + H] = product(both, hi[:, at], lo[:, at], False)
    out[:, 4 * W :] = lanes(row_sums(values * values))


def send_kernel(place, hi, lo, a, b, c, d, state, image, send, image_out, state_out):
    turn = place[3]
    payload = (a[...] + b[...]) + (c[...] + d[...])
    stats = restored(payload[4 * K :])
    payload = jnp.concatenate([payload[c * K : (c + 1) * K] for c in range(4)], 1)
    norm = stats[:, 0:1]
    ratio = norm / state[:, 0:1]
    ratio = jnp.where(turn == 0, 1.0, jnp.where(turn == 1, 0.0, ratio))
    square = norm + ratio * (2.0 * stats[:, 1:2] + ratio * state[:, 1:2])
    values = jnp.where(turn == 0, -1.0, 1.0) * payload + ratio * image[...]
    image_out[...] = values
    state_out[...] = lanes(norm, square, ratio)
    chunks(place, hi, lo, values, -1, 1 - place[2], send)


def keep_kernel(place, hi, lo, state, image, after, direction, keep, direction_out):
    fresh = jnp.where(place[3] == 0, 0.0, 1.0)
    ratio = state[:, 2:3]
    for j in range(Z):
        direction_out[j] = fresh * after[j] + ratio * direction[j]
    chunks(place, hi, lo, image[...], 1, place[2], keep)


VMEM = pl.BlockSpec(memory_space=pltpu.VMEM)
SMEM = pl.BlockSpec(memory_space=pltpu.SMEM)
ANY = pl.BlockSpec(memory_space=pl.ANY)


def array(*shape):
    return jax.ShapeDtypeStruct(shape, jnp.float32)


def call(kernel, kinds, outs, scratch, limit, *args, flops=10**9):
    return pl.pallas_call(
        kernel,
        in_specs=kinds + [VMEM] * (len(args) - len(kinds)),
        out_specs=[VMEM] * len(outs),
        out_shape=outs,
        scratch_shapes=scratch,
        cost_estimate=pl.CostEstimate(flops=flops, transcendentals=0, bytes_accessed=2**23),
        compiler_params=pltpu.CompilerParams(vmem_limit_bytes=limit * 2**20),
    )(*args)


STACK = array(Z, K, W)
TERM = jax.ShapeDtypeStruct((W, Z * W), jnp.bfloat16)
WIDE = array(K, 4 * W + S)


def prepare_kernel(design, hi, lo):
    for i in range(0, W, 64):
        hi[i : i + 64], lo[i : i + 64] = split(design[i : i + 64])


def prepare(design):
    block = pl.BlockSpec((W, 2 * W), lambda j: (0, j))
    return pl.pallas_call(
        prepare_kernel,
        grid=(Z // 2,),
        in_specs=[block],
        out_specs=[block, block],
        out_shape=[TERM, TERM],
        cost_estimate=pl.CostEstimate(flops=10**10, transcendentals=0, bytes_accessed=2**24),
        compiler_params=pltpu.CompilerParams(vmem_limit_bytes=58 * 2**20),
    )(design)


def pack_kernel(place, chip, extra, whole, small):
    tile = flipped(extra[...])
    for c in range(4):
        whole[c * K : (c + 1) * K] = chip[:, c * S : (c + 1) * S]
    whole[4 * K :] = tile
    for c in range(2):
        one, two = chip[:, c * S : (c + 1) * S], chip[:, H + c * S : H + (c + 1) * S]
        small[c * K : (c + 1) * K] = jnp.where(place[2] == 0, one, two)
    small[2 * K :] = tile


def forward(*args):
    scratch = [
        pltpu.VMEM((2 * K, Z * W), jnp.bfloat16),
        pltpu.VMEM((W, 4 * K), jnp.float32),
        pltpu.VMEM((4 * K, W), jnp.float32),
    ]
    return call(forward_kernel, [SMEM], [array(T, S), STACK, array(K, W)], scratch, 24, *args)


def on_device(design, targets, warm_solution, warm_sparse, warm_dual, sparsity):
    z = lax.axis_index("row_0")
    core = lax.axis_index("row_1")

    def place(turn):
        return jnp.stack([z, 1 - 2 * core, core, turn]).astype(jnp.int32)

    def half(x):
        return jnp.where(core == 0, x[:, :H], x[:, H : 2 * H])

    def joined(mine, other):
        return jnp.where(core == 0, jnp.concatenate([mine, other], 1), jnp.concatenate([other, mine], 1))

    def gathered(at, chip, extra):
        outs = [array(T, S), array(2 * K + 8, S)]
        whole, small = call(pack_kernel, [SMEM], outs, [], 24, at, chip, extra, flops=10**11)
        parts = {}
        for k in (4, 3, 2, 1):
            parts[k] = along_z(small if k == 4 else whole, k)
        mine = jnp.concatenate([parts[k] for k in (1, 2, 3, 4)], 0)
        return mine, pair(mine)

    def reduced(both):
        got4 = along_z(both[:, 3 * W : 3 * W + H], 4)
        got3 = along_z(both[:, 2 * W : 3 * W], 3)
        got2 = along_z(both[:, W : 2 * W], 2)
        got1 = along_z(both[:, :W], 1)
        mine = got4 + both[:, 3 * W + H : 4 * W]
        side = (got1 + got2 + got3) + joined(mine, jnp.zeros_like(mine))
        return side + pair(side), both[:, 4 * W :]

    def plane(x):
        a, b, c, d = ring_parts(x, "col_1")
        return ring_parts((a + b) + (c + d), "col_0")

    found = joined(warm_solution, pair(warm_solution))
    shift = penalty * (warm_sparse - warm_dual - warm_solution)
    shift = joined(shift, pair(shift))
    none = jnp.zeros((K, S), jnp.float32)
    stack = jnp.zeros((Z, K, W), jnp.float32)

    hi, lo = prepare(design)

    def ahead(turn, carry):
        chip, part, state, residual, direction, found, _ = carry
        at = place(turn)
        mine, theirs = gathered(at, chip, part)
        value, residual, found = forward(
            at, hi, lo, chip, mine, theirs, state, part, residual, direction, found
        )
        return at, plane(value), residual, found

    def advance(turn, carry):
        at, parts, residual, found = ahead(turn, carry)
        state, direction, image = carry[2], carry[4], carry[6]
        outs = [WIDE, array(K, W), array(K, S)]
        send, image, state = call(send_kernel, [SMEM], outs, [], 24, at, hi, lo, *parts, state, image)
        theirs = pair(send)
        keep, direction = call(
            keep_kernel, [SMEM], [WIDE, STACK], [], 24, at, hi, lo, state, image, residual, direction
        )
        chip, part = reduced(keep + theirs)
        chip = chip + jnp.where(turn == 0, shift, 0.0)
        return chip, part, state, residual, direction, found, image

    carry = lax.fori_loop(0, STEPS, advance, (found, none, none, stack, stack, found, targets))
    state, direction, image = carry[2], carry[4], carry[6]
    _, parts, residual, found = ahead(STEPS, carry)
    payload = (parts[0] + parts[1]) + (parts[2] + parts[3])
    stats = jnp.transpose(payload[4 * K :, :K])
    norm = stats[:, 0:1]
    ratio = norm / state[:, 0:1]
    square = norm + ratio * (2.0 * stats[:, 1:2] + ratio * state[:, 1:2])
    image = jnp.concatenate([payload[c * K : (c + 1) * K] for c in range(4)], 1) + ratio * image
    direction = half(residual[0]) + ratio * half(direction[0])
    part = jnp.pad(row_sums(image * image)[:, 0], (0, S - K))
    sent = lax.all_to_all(jnp.broadcast_to(part, (16, 8, S)), ROW, 0, 0, tiled=True)
    part = jnp.sum(sent, axis=0)[0, :K, None]
    solution = half(found) + norm / (part + penalty * square) * direction

    thresh = (sparsity / penalty)[:, None]
    merged = solution + warm_dual
    sparse = jnp.sign(merged) * jnp.maximum(jnp.abs(merged) - thresh, 0.0)
    return solution, sparse, merged - sparse


def solution(mesh):
    finer = Mesh(mesh.devices.reshape(8, 2, 4, 4), ("row_0", "row_1", "col_0", "col_1"))

    return jax.shard_map(
        on_device,
        mesh=finer,
        in_specs=(
            P(ROW, COL),
            P(None, ROW),
            P(None, COL_ROW),
            P(None, COL_ROW),
            P(None, COL_ROW),
            P(),
        ),
        out_specs=(P(None, COL_ROW), P(None, COL_ROW), P(None, COL_ROW)),
        check_vma=False,
    )
```

```python
import jax
import jax.numpy as jnp
from jax import lax
from jax.experimental import pallas as pl
from jax.experimental.pallas import tpu as pltpu
from jax.sharding import Mesh
from jax.sharding import PartitionSpec as P


STEPS = 3
COL = ("col_0", "col_1")
ROW = ("row_0", "row_1")
COL_ROW = ("col_0", "col_1", "row_0", "row_1")

penalty = 0.5
Z = 8
K = 32
W = 512
H = 256
S = 128
T = 4 * K + 8


def pair(x):
    return lax.ppermute(x, "row_1", [(0, 1), (1, 0)])


def along_z(x, k):
    table = []
    for z in range(Z):
        if k < Z // 2:
            table.append((2 * z, 2 * ((z + k) % Z)))
        table.append((2 * z + 1, 2 * ((z - k) % Z) + 1))
    return lax.ppermute(x, ROW, table)


def ring_parts(x, axis):
    n = 4
    parts = [x]
    for k in (2, 1, 3):
        parts.append(lax.ppermute(x, axis, [(i, (i + k) % n) for i in range(n)]))
    return parts


def split(x):
    hi = x.astype(jnp.bfloat16)
    return hi, (x - hi.astype(jnp.float32)).astype(jnp.bfloat16)


def dot(a, b, transposed):
    dims = (((1,), (1 if transposed else 0,)), ((), ()))
    return lax.dot_general(a, b, dims, preferred_element_type=jnp.float32)


def product(both, hi, lo, transposed):
    wide = dot(both, hi, transposed)
    return (wide[:K] + wide[K:]) + dot(both[:K], lo, transposed)


def columns(place, offset):
    at = lax.rem(place[0] + place[1] * offset + 2 * Z, Z)
    return pl.ds(pl.multiple_of(at * W, W), W)


def lanes(*stats):
    lane = lax.broadcasted_iota(jnp.int32, (K, S), 1)
    out = jnp.zeros((K, S), jnp.float32)
    for i, stat in enumerate(stats):
        out = jnp.where(lane == i, stat, out)
    return out


def flipped(stats):
    return jnp.transpose(jnp.concatenate([stats, jnp.zeros((S - K, S), jnp.float32)], 0))[:8]


def restored(tile):
    return jnp.transpose(jnp.concatenate([tile, jnp.zeros((S - 8, S), jnp.float32)], 0))[:K]


def row_sums(values):
    return jnp.sum(values, axis=1, keepdims=True)


def forward_offset(j):
    return Z - j


def forward_kernel(
    place, hi, lo, chip, mine, theirs, state, part, before, direction, found,
    out, after, found_out, both, acc, top,
):
    early = place[3] < 2
    total = jnp.zeros((8, S), jnp.float32)
    for i in range(4):
        at = slice(i * T + 4 * K, (i + 1) * T)
        total = total + (mine[at] + theirs[at])
    total = part[...] + restored(total)
    alpha = state[:, 0:1] / (total[:, 0:1] + penalty * state[:, 1:2])
    alpha = jnp.where(early, -1.0, alpha)
    kept = jnp.where(early, 0.0, 1.0)
    found_out[...] = found[...] + alpha * direction[0]
    R = 16
    tops = []

    def piece(ref, index, count, i):
        starts = [index * T + c * K + i * R for c in range(count)]
        return jnp.concatenate([ref[at : at + R] for at in starts], 1)

    for i in range(K // R):
        rows = pl.ds(i * R, R)
        squares = crossed = None
        for j in range(Z):
            if j == 0:
                value = chip[rows, :]
            elif j < 4:
                value = piece(mine, j - 1, 4, i)
            elif j > 4:
                value = piece(theirs, 7 - j, 4, i)
            else:
                value = piece(mine, 3, 4, i) + piece(theirs, 3, 4, i)
            old = direction[j, rows, :]
            value = kept * before[j, rows, :] - alpha[i * R : i * R + R] * (value + penalty * old)
            after[j, rows, :] = value
            squares = value * value if squares is None else squares + value * value
            crossed = value * old if crossed is None else crossed + value * old
            big, small = split(value)
            at = columns(place, forward_offset(j))
            both[rows, at] = big
            both[pl.ds(K + i * R, R), at] = small
        tops.append([row_sums(squares), row_sums(crossed)])
    acc[:, : 2 * K] = dot(hi[...], both[...], True)
    acc[:, 2 * K : 3 * K] = dot(lo[...], both[:K], True)
    top[...] = jnp.transpose(acc[...])
    value = (top[:K] + top[K : 2 * K]) + top[2 * K : 3 * K]
    for c in range(4):
        out[c * K : (c + 1) * K] = value[:, c * S : (c + 1) * S]
    out[4 * K :] = flipped(lanes(*[jnp.concatenate(list(pieces), 0) for pieces in zip(*tops)]))


def chunks(place, hi, lo, values, side, which, out):
    both = jnp.concatenate(split(values), 0)
    for i in range(3):
        at = columns(place, side * (i + 1))
        out[:, i * W : (i + 1) * W] = product(both, hi[:, at], lo[:, at], False)
    at = columns(place, Z // 2 * which)
    out[:, 3 * W : 4 * W] = product(both, hi[:, at], lo[:, at], False)
    out[:, 4 * W :] = lanes(row_sums(values * values))


def send_kernel(place, hi, lo, a, b, c, d, state, image, send, image_out, state_out):
    turn = place[3]
    payload = (a[...] + b[...]) + (c[...] + d[...])
    stats = restored(payload[4 * K :])
    payload = jnp.concatenate([payload[c * K : (c + 1) * K] for c in range(4)], 1)
    norm = stats[:, 0:1]
    ratio = norm / state[:, 0:1]
    ratio = jnp.where(turn == 0, 1.0, jnp.where(turn == 1, 0.0, ratio))
    square = norm + ratio * (2.0 * stats[:, 1:2] + ratio * state[:, 1:2])
    values = jnp.where(turn == 0, -1.0, 1.0) * payload + ratio * image[...]
    image_out[...] = values
    state_out[...] = lanes(norm, square, ratio)
    chunks(place, hi, lo, values, -1, 1 - place[2], send)


def keep_kernel(place, hi, lo, state, image, after, direction, keep, direction_out):
    fresh = jnp.where(place[3] == 0, 0.0, 1.0)
    ratio = state[:, 2:3]
    for j in range(Z):
        direction_out[j] = fresh * after[j] + ratio * direction[j]
    chunks(place, hi, lo, image[...], 1, place[2], keep)


VMEM = pl.BlockSpec(memory_space=pltpu.VMEM)
SMEM = pl.BlockSpec(memory_space=pltpu.SMEM)
ANY = pl.BlockSpec(memory_space=pl.ANY)


def array(*shape):
    return jax.ShapeDtypeStruct(shape, jnp.float32)


def call(kernel, kinds, outs, scratch, limit, *args, flops=10**9):
    return pl.pallas_call(
        kernel,
        in_specs=kinds + [VMEM] * (len(args) - len(kinds)),
        out_specs=[VMEM] * len(outs),
        out_shape=outs,
        scratch_shapes=scratch,
        cost_estimate=pl.CostEstimate(flops=flops, transcendentals=0, bytes_accessed=2**23),
        compiler_params=pltpu.CompilerParams(vmem_limit_bytes=limit * 2**20),
    )(*args)


STACK = array(Z, K, W)
TERM = jax.ShapeDtypeStruct((W, Z * W), jnp.bfloat16)
WIDE = array(K, 4 * W + S)


def prepare_kernel(design, hi, lo):
    for i in range(0, W, 64):
        hi[i : i + 64], lo[i : i + 64] = split(design[i : i + 64])


def prepare(design):
    block = pl.BlockSpec((W, 2 * W), lambda j: (0, j))
    return pl.pallas_call(
        prepare_kernel,
        grid=(Z // 2,),
        in_specs=[block],
        out_specs=[block, block],
        out_shape=[TERM, TERM],
        cost_estimate=pl.CostEstimate(flops=10**10, transcendentals=0, bytes_accessed=2**24),
        compiler_params=pltpu.CompilerParams(vmem_limit_bytes=58 * 2**20),
    )(design)


def pack_kernel(chip, extra, whole):
    for c in range(4):
        whole[c * K : (c + 1) * K] = chip[:, c * S : (c + 1) * S]
    whole[4 * K :] = flipped(extra[...])


def forward(*args):
    scratch = [
        pltpu.VMEM((2 * K, Z * W), jnp.bfloat16),
        pltpu.VMEM((W, 4 * K), jnp.float32),
        pltpu.VMEM((4 * K, W), jnp.float32),
    ]
    return call(forward_kernel, [SMEM], [array(T, S), STACK, array(K, W)], scratch, 24, *args)


def on_device(design, targets, warm_solution, warm_sparse, warm_dual, sparsity):
    z = lax.axis_index("row_0")
    core = lax.axis_index("row_1")

    def place(turn):
        return jnp.stack([z, 1 - 2 * core, core, turn]).astype(jnp.int32)

    def half(x):
        return jnp.where(core == 0, x[:, :H], x[:, H : 2 * H])

    def joined(mine, other):
        return jnp.where(core == 0, jnp.concatenate([mine, other], 1), jnp.concatenate([other, mine], 1))

    def gathered(chip, extra):
        (whole,) = call(pack_kernel, [], [array(T, S)], [], 24, chip, extra, flops=10**11)
        parts = {}
        for k in (4, 3, 2, 1):
            parts[k] = along_z(whole, k)
        mine = jnp.concatenate([parts[k] for k in (1, 2, 3, 4)], 0)
        return mine, pair(mine)

    def reduced(both):
        got4 = along_z(both[:, 3 * W : 4 * W], 4)
        got3 = along_z(both[:, 2 * W : 3 * W], 3)
        got2 = along_z(both[:, W : 2 * W], 2)
        got1 = along_z(both[:, :W], 1)
        side = (got1 + got2 + got3) + jnp.where(core == 0, both[:, 3 * W : 4 * W], got4)
        return side + pair(side), both[:, 4 * W :]

    def plane(x):
        a, b, c, d = ring_parts(x, "col_1")
        return ring_parts((a + b) + (c + d), "col_0")

    found = joined(warm_solution, pair(warm_solution))
    shift = penalty * (warm_sparse - warm_dual - warm_solution)
    shift = joined(shift, pair(shift))
    none = jnp.zeros((K, S), jnp.float32)
    stack = jnp.zeros((Z, K, W), jnp.float32)

    hi, lo = prepare(design)

    def ahead(turn, carry):
        chip, part, state, residual, direction, found, _ = carry
        at = place(turn)
        mine, theirs = gathered(chip, part)
        value, residual, found = forward(
            at, hi, lo, chip, mine, theirs, state, part, residual, direction, found
        )
        return at, plane(value), residual, found

    def advance(turn, carry):
        at, parts, residual, found = ahead(turn, carry)
        state, direction, image = carry[2], carry[4], carry[6]
        outs = [WIDE, array(K, W), array(K, S)]
        send, image, state = call(send_kernel, [SMEM], outs, [], 24, at, hi, lo, *parts, state, image)
        theirs = pair(send)
        keep, direction = call(
            keep_kernel, [SMEM], [WIDE, STACK], [], 24, at, hi, lo, state, image, residual, direction
        )
        chip, part = reduced(keep + theirs)
        chip = chip + jnp.where(turn == 0, shift, 0.0)
        return chip, part, state, residual, direction, found, image

    carry = lax.fori_loop(0, STEPS, advance, (found, none, none, stack, stack, found, targets))
    state, direction, image = carry[2], carry[4], carry[6]
    _, parts, residual, found = ahead(STEPS, carry)
    payload = (parts[0] + parts[1]) + (parts[2] + parts[3])
    stats = jnp.transpose(payload[4 * K :, :K])
    norm = stats[:, 0:1]
    ratio = norm / state[:, 0:1]
    square = norm + ratio * (2.0 * stats[:, 1:2] + ratio * state[:, 1:2])
    image = jnp.concatenate([payload[c * K : (c + 1) * K] for c in range(4)], 1) + ratio * image
    direction = half(residual[0]) + ratio * half(direction[0])
    part = jnp.pad(row_sums(image * image)[:, 0], (0, S - K))
    sent = lax.all_to_all(jnp.broadcast_to(part, (16, 8, S)), ROW, 0, 0, tiled=True)
    part = jnp.sum(sent, axis=0)[0, :K, None]
    solution = half(found) + norm / (part + penalty * square) * direction

    thresh = (sparsity / penalty)[:, None]
    merged = solution + warm_dual
    sparse = jnp.sign(merged) * jnp.maximum(jnp.abs(merged) - thresh, 0.0)
    return solution, sparse, merged - sparse


def solution(mesh):
    finer = Mesh(mesh.devices.reshape(8, 2, 4, 4), ("row_0", "row_1", "col_0", "col_1"))

    return jax.shard_map(
        on_device,
        mesh=finer,
        in_specs=(
            P(ROW, COL),
            P(None, ROW),
            P(None, COL_ROW),
            P(None, COL_ROW),
            P(None, COL_ROW),
            P(),
        ),
        out_specs=(P(None, COL_ROW), P(None, COL_ROW), P(None, COL_ROW)),
        check_vma=False,
    )
```
